32 devices in a mesh: dp: 1, sp: 32 (over x, y, z, core).
Axes of the slice: x: 2, y: 2, z: 4, core: 2. Of those that a mesh axis runs over, the one named last changes fastest.
Arguments:
- q: bfloat16 [32, 16, 128], P('dp')
- k: bfloat16 [32, 8192, 16, 128], P('dp', 'sp')
- v: bfloat16 [32, 8192, 16, 128], P('dp', 'sp')
Outputs:
- q: bfloat16 [32, 16, 128], P('dp')
All inputs are finite; a program needn't handle non-finite values.
Results may differ from the reference program's by a relative error of at most 0.012.
Values are sent between devices in bfloat16 or wider.
A program may use at most 2 GiB of HBM per device.

```python
import jax
import jax.numpy as jnp

BATCH = 32
CACHE = 8192
HEADS = 16
KV_HEADS = 16
HEAD = 128


def setup_inputs(seed: int = 0, part: int = 0) -> dict:
    kq, kk, kv = (jax.random.fold_in(k, part) for k in jax.random.split(jax.random.key(seed), 3))
    return {
        "q": (3 * jax.random.normal(kq, (BATCH, HEADS, HEAD), jnp.float32)).astype(jnp.bfloat16),
        "k": jax.random.normal(kk, (BATCH, CACHE, KV_HEADS, HEAD), jnp.float32).astype(jnp.bfloat16),
        "v": jax.random.normal(kv, (BATCH, CACHE, KV_HEADS, HEAD), jnp.float32).astype(jnp.bfloat16),
    }


def einsum(form, a, b):
    return jnp.einsum(form, a.astype(jnp.float32), b.astype(jnp.float32))


def reference(q, k, v):
    grouped = q.reshape(BATCH, KV_HEADS, -1, HEAD)
    scores = einsum("bgsd,bugd->bgsu", grouped, k) * HEAD**-0.5
    weights = jax.nn.softmax(scores, -1).astype(jnp.bfloat16)
    return einsum("bgsu,bugd->bgsd", weights, v).astype(jnp.bfloat16).reshape(BATCH, HEADS, HEAD)
```

```python
import functools

import jax
import jax.numpy as jnp
from jax import lax
from jax.experimental import pallas as pl
from jax.experimental.pallas import tpu as pltpu
from jax.sharding import PartitionSpec as P

MESH = pl.DeviceIdType.MESH
SLOTS = 8
LANES = 128


def kernel(n, scale, q_ref, k_hbm, v_hbm, out_ref, kbuf, vbuf, s0, s1, seen_out, stat_out, seen_in, stat_in, ksem, vsem, seen_ssem, stat_ssem, seen_rsem, stat_rsem, out_ssem, out_rsem):
    me = lax.axis_index("sp")
    batch, tokens, heads, head = k_hbm.shape
    half = tokens * heads // 2
    slots = kbuf.shape[0]
    bits = (n - 1).bit_length()

    def peer(x):
        there = me
        for bit in range(bits):
            mine, flip = (me // 2**bit) % 2, (x // 2**bit) % 2
            there = there + flip * (1 - 2 * mine) * 2**bit
        return there

    def owner(i):
        return peer(n - 1 - i)

    def copy_k(i):
        slot = lax.rem(i, slots)
        return pltpu.make_async_copy(k_hbm.at[owner(i)], kbuf.at[slot], ksem.at[slot])

    def copy_v(i):
        slot = lax.rem(i, slots)
        return pltpu.make_async_copy(v_hbm.at[owner(i)], vbuf.at[slot], vsem.at[slot])

    def send_seen(x, there):
        return pltpu.make_async_remote_copy(seen_out.at[x], seen_in.at[x], seen_ssem.at[x], seen_rsem.at[x], device_id={"sp": there}, device_id_type=MESH)

    def send_stat(x, there):
        return pltpu.make_async_remote_copy(stat_out.at[x], stat_in.at[x], stat_ssem.at[x], stat_rsem.at[x], device_id={"sp": there}, device_id_type=MESH)

    def send_out(x, there):
        return pltpu.make_async_remote_copy(out_ref.at[me], out_ref.at[me], out_ssem.at[x], out_rsem.at[x], device_id={"sp": there}, device_id_type=MESH)

    copy_k(0).start()
    for i in range(slots - 1):
        copy_k(i + 1).start()
        copy_v(i).start()
    copy_v(slots - 1).start()

    barrier = pltpu.get_barrier_semaphore()

    @pl.loop(1, n)
    def _(x):
        pl.semaphore_signal(barrier, inc=1, device_id={"sp": peer(x)}, device_id_type=MESH)

    rows = lax.broadcasted_iota(jnp.int32, (2 * heads, LANES), 0)
    lanes = lax.broadcasted_iota(jnp.int32, (2 * heads, LANES), 1)
    bias = jnp.where(rows % heads == lanes % heads, 0.0, -jnp.inf).astype(jnp.float32)
    factor = scale * 1.4426950408889634

    def scores(i, s_ref):
        q = q_ref[owner(i)]
        zero = jnp.zeros_like(q)
        q2 = jnp.concatenate([jnp.concatenate([q, zero], 1), jnp.concatenate([zero, q], 1)], 0)
        k = kbuf[lax.rem(i, slots)].reshape(2, half, head)
        k2 = jnp.concatenate([k[0], k[1]], 1)
        s_ref[...] = lax.dot_general(q2, k2, (((1,), (1,)), ((), ())), preferred_element_type=jnp.float32)

    def weigh(s_ref):
        tiles = [s_ref[:, t : t + LANES] + bias for t in range(0, half, LANES)]
        high = functools.reduce(jnp.maximum, tiles)
        high = jnp.max(jnp.maximum(high[:heads], high[heads:]), 1, keepdims=True)
        both = jnp.concatenate([high, high], 0)
        weights = [jnp.exp2((t - both) * factor) for t in tiles]
        total = functools.reduce(jnp.add, weights)
        total = jnp.sum(total[:heads] + total[heads:], 1, keepdims=True)
        return jnp.concatenate([w.astype(jnp.bfloat16) for w in weights], 1), high, total

    def values(i, weights):
        v = vbuf[lax.rem(i, slots)].reshape(2, half, head)
        v2 = jnp.concatenate([v[0], v[1]], 1)
        seen = jnp.dot(weights, v2, preferred_element_type=jnp.float32)
        return seen[:heads, :head] + seen[heads:, head:]

    lane = lax.broadcasted_iota(jnp.int32, (heads // 2, LANES), 1)

    def part(i, s_ref):
        weights, high, total = weigh(s_ref)
        seen = values(i, weights)
        x = n - 1 - i
        h = heads // 2
        seen_out[x] = seen.astype(jnp.bfloat16)
        stat_out[x] = jnp.where(lane < 32, high[:h], jnp.where(lane < 64, high[h:], jnp.where(lane < 96, total[:h], total[h:])))
        there = peer(x)
        send_seen(x, there).start()
        send_stat(x, there).start()

    def step(i, s_now, s_next):
        copy_k(i + 1).wait()
        scores(i + 1, s_next)
        copy_v(i).wait()
        part(i, s_now)

    def refill(i):
        @pl.when(i + slots < n)
        def _():
            copy_k(i + slots).start()

        @pl.when((i >= 1) & (i - 1 + slots < n))
        def _():
            copy_v(i - 1 + slots).start()

    copy_k(0).wait()
    scores(0, s0)
    pl.semaphore_wait(barrier, n - 1)

    @pl.loop(0, n // 2 - 1)
    def _(j):
        i = 2 * j
        refill(i)
        step(i, s0, s1)
        refill(i + 1)
        step(i + 1, s1, s0)

    i = n - 2
    step(i, s0, s1)

    weights, high, total = weigh(s1)
    copy_v(n - 1).wait()
    seen = values(n - 1, weights)

    @pl.loop(1, n)
    def _(x):
        there = peer(x)
        send_stat(x, there).wait_recv()
        send_seen(x, there).wait_recv()

    top = functools.reduce(jnp.maximum, [stat_in[x] for x in range(1, n)])
    sums = jnp.zeros((heads // 2, LANES), jnp.float32)
    acc = jnp.zeros((heads, head), jnp.float32)
    for x in range(1, n):
        stat = stat_in[x]
        w = jnp.exp2((stat - top) * factor)
        sums += pltpu.roll(w, LANES // 2, 1) * stat
        acc += seen_in[x].astype(jnp.float32) * jnp.concatenate([w[:, 0:1], w[:, 32:33]], 0)
    top = jnp.concatenate([top[:, 0:1], top[:, 32:33]], 0)
    sums = jnp.concatenate([sums[:, 64:65], sums[:, 96:97]], 0)
    new = jnp.maximum(top, high)
    theirs, mine = jnp.exp2((top - new) * factor), jnp.exp2((high - new) * factor)
    result = (acc * theirs + seen * mine) / (sums * theirs + total * mine)
    out_ref[me] = result.astype(jnp.bfloat16)

    @pl.loop(0, n - 1)
    def _(i):
        send_out(n - 1 - i, owner(i)).start()

    @pl.loop(1, n)
    def _(x):
        there = peer(x)
        copy = send_out(x, there)
        copy.wait_send()
        send_seen(x, there).wait_send()
        send_stat(x, there).wait_send()
        pltpu.make_async_remote_copy(out_ref.at[there], out_ref.at[there], out_ssem.at[x], out_rsem.at[x], device_id={"sp": there}, device_id_type=MESH).wait_recv()


def solution(mesh):
    n = mesh.shape["sp"]

    def step(q, k, v):
        batch, tokens, heads, head = k.shape
        rows = tokens * heads // 2
        return pl.pallas_call(
            functools.partial(kernel, n, head**-0.5),
            out_shape=jax.ShapeDtypeStruct(q.shape, q.dtype),
            in_specs=[pl.BlockSpec(memory_space=pltpu.VMEM), pl.BlockSpec(memory_space=pl.ANY), pl.BlockSpec(memory_space=pl.ANY)],
            out_specs=pl.BlockSpec(memory_space=pltpu.VMEM),
            scratch_shapes=[
                pltpu.VMEM((SLOTS, tokens, heads, head), k.dtype),
                pltpu.VMEM((SLOTS, tokens, heads, head), v.dtype),
                pltpu.VMEM((2 * heads, rows), jnp.float32),
                pltpu.VMEM((2 * heads, rows), jnp.float32),
                pltpu.VMEM((n, heads, head), jnp.bfloat16),
                pltpu.VMEM((n, heads // 2, LANES), jnp.float32),
                pltpu.VMEM((n, heads, head), jnp.bfloat16),
                pltpu.VMEM((n, heads // 2, LANES), jnp.float32),
                pltpu.SemaphoreType.DMA((SLOTS,)),
                pltpu.SemaphoreType.DMA((SLOTS,)),
                pltpu.SemaphoreType.DMA((n,)),
                pltpu.SemaphoreType.DMA((n,)),
                pltpu.SemaphoreType.DMA((n,)),
                pltpu.SemaphoreType.DMA((n,)),
                pltpu.SemaphoreType.DMA((n,)),
                pltpu.SemaphoreType.DMA((n,)),
            ],
            compiler_params=pltpu.CompilerParams(collective_id=0, has_side_effects=True, vmem_limit_bytes=60 * 2**20),
        )(q, k, v)

    return jax.shard_map(
        step,
        mesh=mesh,
        in_specs=(P("dp", None, None), P("dp", "sp", None, None), P("dp", "sp", None, None)),
        out_specs=P("dp", None, None),
        check_vma=False,
    )
```

```python
import functools

import jax
import jax.numpy as jnp
from jax import lax
from jax.experimental import pallas as pl
from jax.experimental.pallas import tpu as pltpu
from jax.sharding import PartitionSpec as P

MESH = pl.DeviceIdType.MESH
SLOTS = 4
UNROLL = 4
GREET = 8
PIECES = 4
LANES = 128


def kernel(n, scale, q_hbm, k_hbm, v_hbm, out_ref, q_ref, kbuf, vbuf, s0, s1, seen_out, stat_out, seen_in, stat_in, acc_ref, top_ref, sums_ref, mine, qsem, ksem, vsem, psem, part_ssem, seen_rsem, stat_rsem, out_ssem, out_rsem):
    me = lax.axis_index("sp")
    batch, _, tokens, heads, head = k_hbm.shape
    half = tokens * heads
    bits = (n - 1).bit_length()
    low = UNROLL.bit_length() - 1
    turn = [(1 - 2 * ((me // 2**b) % 2)) * 2**b for b in range(bits)]
    groups = [range(2**b, 2 ** (b + 1)) for b in range(1, bits)]
    groups[0] = range(1, 4)

    def group_of(x):
        return max(x.bit_length() - 2, 0)

    def peer(x):
        return sum((turn[b] for b in range(bits) if x >> b & 1), me)

    def block(j):
        if isinstance(j, int):
            return peer((n - 1 - UNROLL * j) >> low << low)
        there, rest = me, n // UNROLL - 1 - j
        for b in range(bits - 1, low - 1, -1):
            bit = rest // 2 ** (b - low)
            there, rest = there + bit * turn[b], rest - bit * 2 ** (b - low)
        return there

    def at(base, r):
        x = UNROLL - 1 - r
        return sum((turn[b] for b in range(low) if x >> b & 1), base)

    def copy_k(owner, slot):
        return pltpu.make_async_copy(k_hbm.at[owner], kbuf.at[slot], ksem.at[slot])

    def copy_v(owner, slot):
        return pltpu.make_async_copy(v_hbm.at[owner], vbuf.at[slot], vsem.at[slot])

    def copy_piece(owner, slot, p):
        run = pl.ds(p * (tokens // PIECES), tokens // PIECES)
        return pltpu.make_async_copy(v_hbm.at[owner, :, run], vbuf.at[slot, :, run], psem.at[p])

    def remote(src, dst, ssem, rsem, there):
        return pltpu.make_async_remote_copy(src, dst, ssem, rsem, device_id={"sp": there}, device_id_type=MESH)

    def send_part(x, there, group):
        remote(seen_out.at[x], seen_in.at[x], part_ssem.at[0], seen_rsem.at[group], there).start()
        remote(stat_out.at[x], stat_in.at[x], part_ssem.at[1], stat_rsem.at[group], there).start()

    q_copy = pltpu.make_async_copy(q_hbm, q_ref, qsem)
    first = [peer(n - 1 - i) for i in range(SLOTS)]
    q_copy.start()
    copy_k(first[0], 0).start()
    for i in range(SLOTS - 1):
        copy_k(first[i + 1], i + 1).start()
        copy_v(first[i], i).start()
    copy_v(first[-1], SLOTS - 1).start()

    barrier = pltpu.get_barrier_semaphore()
    for x in range(1, n):
        pl.semaphore_signal(barrier, inc=1, device_id={"sp": peer(x)}, device_id_type=MESH)

    rows = lax.broadcasted_iota(jnp.int32, (2 * heads, LANES), 0)
    lanes = lax.broadcasted_iota(jnp.int32, (2 * heads, LANES), 1)
    bias = jnp.where(rows % heads == lanes % heads, 0.0, -jnp.inf).astype(jnp.float32)
    lane = lax.broadcasted_iota(jnp.int32, (heads // 2, LANES), 1)
    factor = scale * 1.4426950408889634

    def scores(owner, slot, s_ref):
        q = q_ref[owner]
        zero = jnp.zeros_like(q)
        q2 = jnp.concatenate([jnp.concatenate([q, zero], 1), jnp.concatenate([zero, q], 1)], 0)
        k = kbuf[slot].reshape(2, half, head)
        k2 = jnp.concatenate([k[0], k[1]], 1)
        s_ref[...] = lax.dot_general(q2, k2, (((1,), (1,)), ((), ())), preferred_element_type=jnp.float32)

    def weigh(s_ref):
        tiles = [s_ref[:, t : t + LANES] + bias for t in range(0, half, LANES)]
        high = functools.reduce(jnp.maximum, tiles)
        high = jnp.max(jnp.maximum(high[:heads], high[heads:]), 1, keepdims=True)
        both = jnp.concatenate([high, high], 0)
        weights = [jnp.exp2((t - both) * factor) for t in tiles]
        total = functools.reduce(jnp.add, weights)
        total = jnp.sum(total[:heads] + total[heads:], 1, keepdims=True)
        return jnp.concatenate([w.astype(jnp.bfloat16) for w in weights], 1), high, total

    def values(slot, weights, p=0, pieces=1):
        run = tokens // pieces
        v = vbuf[slot, :, p * run : (p + 1) * run].reshape(2, run * heads, head)
        v2 = jnp.concatenate([v[0], v[1]], 1)
        weights = weights[:, p * run * heads : (p + 1) * run * heads]
        seen = jnp.dot(weights, v2, preferred_element_type=jnp.float32)
        return seen[:heads, :head] + seen[heads:, head:]

    def part(slot, s_ref, x):
        weights, high, total = weigh(s_ref)
        seen = values(slot, weights)
        h = heads // 2
        seen_out[x] = seen.astype(jnp.bfloat16)
        stat_out[x] = jnp.where(lane < 32, high[:h], jnp.where(lane < 64, high[h:], jnp.where(lane < 96, total[:h], total[h:])))

    def wait_group(g):
        xs = pl.ds(groups[g].start, len(groups[g]))
        remote(stat_in.at[xs], stat_in.at[xs], part_ssem.at[1], stat_rsem.at[g], me).wait_recv()
        remote(seen_in.at[xs], seen_in.at[xs], part_ssem.at[0], seen_rsem.at[g], me).wait_recv()

    def spread(w, at):
        return jnp.concatenate([w[:, at : at + 1], w[:, at + 32 : at + 33]], 0)

    def absorb(g):
        stats = [stat_in[x] for x in groups[g]]
        top = functools.reduce(jnp.maximum, stats)
        sums = jnp.zeros((heads // 2, LANES), jnp.float32)
        acc = jnp.zeros((heads, head), jnp.float32)
        if g < len(groups) - 1:
            old = top_ref[...]
            top = jnp.maximum(top, old)
            w = jnp.exp2((old - top) * factor)
            sums = pltpu.roll(w, LANES // 2, 1) * sums_ref[...]
            acc = acc_ref[...] * spread(w, 0)
        for x, stat in zip(groups[g], stats):
            w = jnp.exp2((stat - top) * factor)
            sums += pltpu.roll(w, LANES // 2, 1) * stat
            acc += seen_in[x].astype(jnp.float32) * spread(w, 0)
        top_ref[...], sums_ref[...], acc_ref[...] = top, sums, acc

    def step(r, bases, s_now, s_next, slot, x, refill, pieces=False, group=None, send=None, sync=None):
        now, after, later = bases
        nxt = at(now, r + 1) if r + 1 < UNROLL else at(after, 0)
        k_slot = (slot + 1) % SLOTS if isinstance(slot, int) else (slot + 1 if (r + 1) % UNROLL else UNROLL - (slot - r))
        if refill:
            copy_k(at(later, r), slot).start()
            before = (slot - 1) % SLOTS if isinstance(slot, int) else (slot - 1 if r else 2 * UNROLL - 1 - slot)
            if r:
                copy_v(at(later, r - 1), before).start()
        with jax.named_scope("wait"):
            copy_k(nxt, k_slot).wait()
            copy_v(at(now, r), slot).wait()
            if group is not None:
                wait_group(group)
        with jax.named_scope("body"):
            scores(nxt, k_slot, s_next)
            part(slot, s_now, x)
            if group is not None:
                absorb(group)
        if refill and r == UNROLL - 1:
            copy_v(at(later, r), slot).start()
        if send is not None:
            send_part(x, at(now, r), send)

    with jax.named_scope("wait0"):
        q_copy.wait()
        copy_k(first[0], 0).wait()
    with jax.named_scope("score0"):
        scores(first[0], 0, s0)

    def steps(j, bases, refill, send, slot0):
        for r in range(UNROLL):
            x = n - 1 - (UNROLL * j + r)
            group = None
            if send:
                group = group_of(x) if isinstance(x, int) else send(j)
            step(r, bases, (s0, s1)[r % 2], (s0, s1)[(r + 1) % 2], slot0 + r, x, refill, send=group)

    for j in range(GREET // UNROLL):
        steps(j, (block(j), block(j + 1), block(j + SLOTS // UNROLL)), True, None, UNROLL * j % SLOTS)

    with jax.named_scope("barrier"):
        pl.semaphore_wait(barrier, n - 1)
    for i in range(GREET):
        x = n - 1 - i
        send_part(x, peer(x), group_of(x))

    for j in range(GREET // UNROLL, n // UNROLL):
        bases = (block(j), block(j + 1) if UNROLL * (j + 1) < n else None, block(j + SLOTS // UNROLL) if UNROLL * (j + SLOTS // UNROLL) < n else None)
        for r in range(UNROLL):
            i = UNROLL * j + r
            x = n - 1 - i
            if i == n - 1:
                break
            group = {n - 8: len(groups) - 1, n - 4: len(groups) - 2, n - 2: len(groups) - 3}.get(i)
            slot = i % SLOTS
            step(r, bases, (s0, s1)[r % 2], (s0, s1)[(r + 1) % 2], slot, x, bases[2] is not None, group=group, send=group_of(x))

    last = (n - 1) % SLOTS
    with jax.named_scope("ownweigh"):
        weights, high, total = weigh(s1)
    with jax.named_scope("waitparts"):
        wait_group(0)
    with jax.named_scope("combine"):
        absorb(0)
        top, sums = spread(top_ref[...], 0), spread(sums_ref[...], 64)
        new = jnp.maximum(top, high)
        theirs, ours = jnp.exp2((top - new) * factor), jnp.exp2((high - new) * factor)
        below = 1 / (sums * theirs + total * ours)
        acc, ours = acc_ref[...] * (theirs * below), ours * below
    with jax.named_scope("waitv"):
        copy_v(me, last).wait()
    with jax.named_scope("ownvalues"):
        mine[...] = (acc + values(last, weights) * ours).astype(jnp.bfloat16)

    with jax.named_scope("sendout"):
        for x in range(n - 1, 0, -1):
            remote(mine, out_ref.at[me], out_ssem, out_rsem, peer(x)).start()
        out_ref[me] = mine[...]

    with jax.named_scope("waitout"):
        every = pl.ds(1, n - 1)
        remote(seen_out.at[every], seen_out.at[every], part_ssem.at[0], out_rsem, me).wait_send()
        remote(stat_out.at[every], stat_out.at[every], part_ssem.at[1], out_rsem, me).wait_send()
        remote(out_ref.at[every], out_ref.at[every], out_ssem, out_rsem, me).wait()


def solution(mesh):
    n = mesh.shape["sp"]

    def step(q, k, v):
        batch, tokens, heads, head = k.shape
        shape = (batch, 2, tokens // 2, heads, head)
        rows = tokens * heads // 2
        return pl.pallas_call(
            functools.partial(kernel, n, head**-0.5),
            out_shape=pltpu.VMEM(q.shape, q.dtype),
            in_specs=[pl.BlockSpec(memory_space=pl.ANY)] * 3,
            out_specs=pl.BlockSpec(memory_space=pltpu.VMEM),
            scratch_shapes=[
                pltpu.VMEM(q.shape, q.dtype),
                pltpu.VMEM((SLOTS, *shape[1:]), k.dtype),
                pltpu.VMEM((SLOTS, *shape[1:]), v.dtype),
                pltpu.VMEM((2 * heads, rows), jnp.float32),
                pltpu.VMEM((2 * heads, rows), jnp.float32),
                pltpu.VMEM((n, heads, head), jnp.bfloat16),
                pltpu.VMEM((n, heads // 2, LANES), jnp.float32),
                pltpu.VMEM((n, heads, head), jnp.bfloat16),
                pltpu.VMEM((n, heads // 2, LANES), jnp.float32),
                pltpu.VMEM((heads, head), jnp.float32),
                pltpu.VMEM((heads // 2, LANES), jnp.float32),
                pltpu.VMEM((heads // 2, LANES), jnp.float32),
                pltpu.VMEM((heads, head), jnp.bfloat16),
                pltpu.SemaphoreType.DMA,
                pltpu.SemaphoreType.DMA((SLOTS,)),
                pltpu.SemaphoreType.DMA((SLOTS,)),
                pltpu.SemaphoreType.DMA((PIECES,)),
                pltpu.SemaphoreType.DMA((2,)),
                pltpu.SemaphoreType.DMA((4,)),
                pltpu.SemaphoreType.DMA((4,)),
                pltpu.SemaphoreType.DMA,
                pltpu.SemaphoreType.DMA,
            ],
            compiler_params=pltpu.CompilerParams(collective_id=0, has_side_effects=True, vmem_limit_bytes=60 * 2**20),
        )(q, k.reshape(shape), v.reshape(shape))

    return jax.shard_map(
        step,
        mesh=mesh,
        in_specs=(P("dp", None, None), P("dp", "sp", None, None), P("dp", "sp", None, None)),
        out_specs=P("dp", None, None),
        check_vma=False,
    )
```

```python
import functools

import jax
import jax.numpy as jnp
from jax import lax
from jax.experimental import pallas as pl
from jax.experimental.pallas import tpu as pltpu
from jax.sharding import PartitionSpec as P

MESH = pl.DeviceIdType.MESH
K_SLOTS = 10
V_SLOTS = 10
GREET = 16
RUN = 2
BUFFERS = 4
FIRST = 2
PHASES = 2
LANES = 128


def distance(x):
    return bin(x >> 3).count("1") + (x >> 1 & 3)


def order_of(n):
    tail = [x for x in (2, 8, 3, 9, 16, 17, 1, 0) if x < n]
    return sorted((x for x in range(n) if x not in tail), key=lambda x: (-distance(x), -x)) + tail


def kernel(n, scale, q_hbm, k_hbm, v_hbm, out_ref, q_ref, kbuf, vbuf, s_refs, p_refs, seen_out, stat_out, seen_in, stat_in, acc_ref, top_ref, sums_ref, own_ref, mine, qsem, ksem, vsem, part_ssem, seen_rsem, stat_rsem, out_ssem, out_rsem):
    me = lax.axis_index("sp")
    batch, tokens, phases, heads, head = k_hbm.shape
    half = tokens * heads // 2
    units = n * phases
    bits = (n - 1).bit_length()
    order = order_of(n)
    turn = [(1 - 2 * ((me // 2**b) % 2)) * 2**b for b in range(bits)]
    sizes = [1, 1] + [RUN] * ((units - 6) // RUN) + [1] * 4
    assert sum(sizes) == units
    starts = [sum(sizes[:b]) for b in range(len(sizes) + 1)]
    blocks = [list(range(a, b)) for a, b in zip(starts, starts[1:])] + [[], []]
    cuts = [0, n // 2, n - n // 4, n]

    def peer(x):
        return sum((turn[b] for b in range(bits) if x >> b & 1), me)

    def owner(u):
        return peer(order[u % n])

    def group_of(i):
        return sum(i >= cut for cut in cuts[1:-1])

    def copy_k(u):
        slot = u % K_SLOTS
        return pltpu.make_async_copy(k_hbm.at[owner(u), :, u // n], kbuf.at[slot], ksem.at[slot])

    def copy_v(u):
        slot = u % V_SLOTS
        return pltpu.make_async_copy(v_hbm.at[owner(u), :, u // n], vbuf.at[slot], vsem.at[slot])

    def remote(src, dst, ssem, rsem, there):
        return pltpu.make_async_remote_copy(src, dst, ssem, rsem, device_id={"sp": there}, device_id_type=MESH)

    def send_part(u):
        f, i = divmod(u, n)
        g, row = group_of(i), pl.ds(i, 1)
        remote(stat_out.at[f, row], stat_in.at[f, row], part_ssem.at[1], stat_rsem.at[f, g], owner(u)).start()
        remote(seen_out.at[f, i], seen_in.at[f, i], part_ssem.at[0], seen_rsem.at[f, g], owner(u)).start()

    q_copy = pltpu.make_async_copy(q_hbm, q_ref, qsem)
    q_copy.start()
    stream = [(copy_k, u) for u in blocks[0] + blocks[1]]
    for b in range(len(sizes)):
        stream += [(copy_k, u) for u in blocks[b + 2]] + [(copy_v, u) for u in blocks[b]]
    stream = [(copy, u) for copy, u in stream if u < (K_SLOTS if copy is copy_k else V_SLOTS)]
    for copy, u in stream[:3]:
        copy(u).start()

    barrier = pltpu.get_barrier_semaphore()
    for x in range(1, n):
        pl.semaphore_signal(barrier, inc=1, device_id={"sp": peer(x)}, device_id_type=MESH)

    for copy, u in stream[3:]:
        copy(u).start()

    rows = lax.broadcasted_iota(jnp.int32, (2 * heads, LANES), 0)
    lanes = lax.broadcasted_iota(jnp.int32, (2 * heads, LANES), 1)
    bias = jnp.where(rows % heads == lanes % heads, 0.0, -jnp.inf).astype(jnp.float32)
    sub = lax.broadcasted_iota(jnp.int32, (heads, LANES), 0)
    lane = lax.broadcasted_iota(jnp.int32, (heads, LANES), 1)
    factor = scale * 1.4426950408889634

    def scores(u):
        f = u // n
        q = q_ref[owner(u)].astype(jnp.float32)[f * heads : (f + 1) * heads]
        zero = jnp.zeros_like(q)
        q2 = jnp.concatenate([jnp.concatenate([q, zero], 1), jnp.concatenate([zero, q], 1)], 0).astype(jnp.bfloat16)
        k = kbuf[u % K_SLOTS].reshape(2, half, head)
        k2 = jnp.concatenate([k[0], k[1]], 1)
        s_refs[u % BUFFERS][...] = lax.dot_general(q2, k2, (((1,), (1,)), ((), ())), preferred_element_type=jnp.float32)

    def weigh(u):
        f, i = divmod(u, n)
        s_ref, p_ref = s_refs[u % BUFFERS], p_refs[u % BUFFERS]
        tiles = [s_ref[:, t : t + LANES] + bias for t in range(0, half, LANES)]
        high = functools.reduce(jnp.maximum, tiles)
        high = jnp.max(jnp.maximum(high[:heads], high[heads:]), 1, keepdims=True)
        both = jnp.concatenate([high, high], 0)
        weights = [jnp.exp2((t - both) * factor) for t in tiles]
        total = functools.reduce(jnp.add, weights)
        total = jnp.sum(total[:heads] + total[heads:], 1, keepdims=True)
        for t, w in enumerate(weights):
            p_ref[:, t * LANES : (t + 1) * LANES] = w.astype(jnp.bfloat16)
        stat = jnp.sum(jnp.where(lane == sub, high, jnp.where(lane == sub + heads, total, 0.0)), 0, keepdims=True)
        if i == n - 1:
            stat_in[f, i : i + 1] = stat
        else:
            stat_out[f, i : i + 1] = stat

    def values(u):
        v = vbuf[u % V_SLOTS].reshape(2, half, head)
        v2 = jnp.concatenate([v[0], v[1]], 1)
        seen = jnp.dot(p_refs[u % BUFFERS][...], v2, preferred_element_type=jnp.float32)
        return seen[:heads, :head] + seen[heads:, head:]

    def wait_group(f, g):
        run = pl.ds(cuts[g], min(cuts[g + 1], n - 1) - cuts[g])
        remote(stat_in.at[f, run], stat_in.at[f, run], part_ssem.at[1], stat_rsem.at[f, g], me).wait_recv()
        remote(seen_in.at[f, run], seen_in.at[f, run], part_ssem.at[0], seen_rsem.at[f, g], me).wait_recv()

    def column(row, first=0):
        return jnp.sum(jnp.where(lane == sub + first, row, 0.0), 1, keepdims=True)

    def absorb(f, g):
        stats = stat_in[f, cuts[g] : cuts[g + 1]]
        top = jnp.max(stats, 0, keepdims=True)
        if g:
            old = top_ref[f]
            top = jnp.maximum(top, old)
        w = jnp.exp2((stats - top) * factor)
        sums = jnp.sum(pltpu.roll(w, heads, 1) * stats, 0, keepdims=True)
        acc = jnp.zeros((heads, head), jnp.float32)
        if g:
            scaled = jnp.exp2((old - top) * factor)
            sums += pltpu.roll(scaled, heads, 1) * sums_ref[f]
            acc = acc_ref[f] * column(scaled)
        for i in range(cuts[g], min(cuts[g + 1], n - 1)):
            row = i - cuts[g]
            acc += seen_in[f, i].astype(jnp.float32) * column(w[row : row + 1])
        if cuts[g + 1] < n:
            top_ref[f], sums_ref[f], acc_ref[f] = top, sums, acc
            return None
        below = 1 / column(sums, heads)
        return acc * below, column(w[n - 1 - cuts[g] : n - cuts[g]]) * below

    def finish(f):
        run = pl.ds(f * heads, heads)

        def send(there):
            remote(mine.at[f], out_ref.at[me, run], out_ssem, out_rsem.at[f], there).start()

        for there in range(FIRST):
            pl.when(me != there)(functools.partial(send, there))
        for x in order[:-1]:
            there = peer(x)
            pl.when(there >= FIRST)(functools.partial(send, there))
        out_ref[me, run] = mine[f]

    def refill(ks, vs):
        for u in ks:
            if u + K_SLOTS < units:
                copy_k(u + K_SLOTS).start()
        for u in vs:
            if u + V_SLOTS < units:
                copy_v(u + V_SLOTS).start()

    with jax.named_scope("wait0"):
        q_copy.wait()
        for u in blocks[0]:
            copy_k(u).wait()
    with jax.named_scope("score0"):
        for u in blocks[0]:
            scores(u)
    refill(blocks[0], [])
    with jax.named_scope("wait1"):
        for u in blocks[1]:
            copy_k(u).wait()
    with jax.named_scope("score1"):
        for u in blocks[1]:
            scores(u)
        for u in blocks[0]:
            weigh(u)

    spare = {n + 12: (0, 0), n + 13: (0, 1), n + 15: (0, 2), units - 2: (1, 0)}
    sent = 0
    for b in range(len(sizes)):
        now, soon, later = blocks[b : b + 3]
        if now[0] >= GREET and not sent:
            with jax.named_scope("barrier"):
                pl.semaphore_wait(barrier, n - 1)
            for u in range(now[0]):
                send_part(u)
            sent = now[0]
        refill(soon, blocks[b - 1] if b else [])
        groups = [spare[u] for u in now if u in spare]
        with jax.named_scope("wait"):
            for u in later:
                copy_k(u).wait()
            for u in now:
                copy_v(u).wait()
            for group in groups:
                wait_group(*group)
        with jax.named_scope("body"):
            for u in now:
                f, i = divmod(u, n)
                seen = values(u)
                if i < n - 1:
                    seen_out[f, i] = seen.astype(jnp.bfloat16)
                else:
                    own_ref[...] = seen
            for u in soon:
                weigh(u)
            for u in later:
                scores(u)
            for group in groups:
                done = absorb(*group)
                if done is not None:
                    mine[group[0]] = (done[0] + own_ref[...] * done[1]).astype(jnp.bfloat16)
        if sent:
            for u in now:
                if u % n < n - 1:
                    send_part(u)
        for group in groups:
            if group[1] == 2:
                finish(group[0])

    with jax.named_scope("waitparts1"):
        wait_group(phases - 1, 1)
    with jax.named_scope("combine1"):
        absorb(phases - 1, 1)
    with jax.named_scope("waitparts"):
        wait_group(phases - 1, 2)
    with jax.named_scope("combine"):
        rest, share = absorb(phases - 1, 2)
        mine[phases - 1] = (rest + own_ref[...] * share).astype(jnp.bfloat16)
    with jax.named_scope("sendout"):
        finish(phases - 1)

    with jax.named_scope("waitout"):
        every = pl.ds(0, n - 1)
        for f in range(phases):
            remote(seen_out.at[f, every], seen_out.at[f, every], part_ssem.at[0], out_rsem.at[f], me).wait_send()
            remote(stat_out.at[f, every], stat_out.at[f, every], part_ssem.at[1], out_rsem.at[f], me).wait_send()
        for f in range(phases):
            landed = out_ref.at[every, pl.ds(f * heads, heads)]
            remote(landed, landed, out_ssem, out_rsem.at[f], me).wait()


def solution(mesh):
    n = mesh.shape["sp"]

    def step(q, k, v):
        batch, tokens, heads, head = k.shape
        heads //= PHASES
        half = tokens * heads // 2
        shape = (batch, tokens, PHASES, heads, head)
        return pl.pallas_call(
            functools.partial(kernel, n, head**-0.5),
            out_shape=pltpu.VMEM(q.shape, q.dtype),
            in_specs=[pl.BlockSpec(memory_space=pl.ANY)] * 3,
            out_specs=pl.BlockSpec(memory_space=pltpu.VMEM),
            scratch_shapes=[
                pltpu.VMEM(q.shape, q.dtype),
                pltpu.VMEM((K_SLOTS, tokens, heads, head), k.dtype),
                pltpu.VMEM((V_SLOTS, tokens, heads, head), v.dtype),
                [pltpu.VMEM((2 * heads, half), jnp.float32)] * BUFFERS,
                [pltpu.VMEM((2 * heads, half), jnp.bfloat16)] * BUFFERS,
                pltpu.VMEM((PHASES, n, heads, head), jnp.bfloat16),
                pltpu.VMEM((PHASES, n, LANES), jnp.float32),
                pltpu.VMEM((PHASES, n, heads, head), jnp.bfloat16),
                pltpu.VMEM((PHASES, n, LANES), jnp.float32),
                pltpu.VMEM((PHASES, heads, head), jnp.float32),
                pltpu.VMEM((PHASES, 1, LANES), jnp.float32),
                pltpu.VMEM((PHASES, 1, LANES), jnp.float32),
                pltpu.VMEM((heads, head), jnp.float32),
                pltpu.VMEM((PHASES, heads, head), jnp.bfloat16),
                pltpu.SemaphoreType.DMA,
                pltpu.SemaphoreType.DMA((K_SLOTS,)),
                pltpu.SemaphoreType.DMA((V_SLOTS,)),
                pltpu.SemaphoreType.DMA((2,)),
                pltpu.SemaphoreType.DMA((PHASES, 3)),
                pltpu.SemaphoreType.DMA((PHASES, 3)),
                pltpu.SemaphoreType.DMA,
                pltpu.SemaphoreType.DMA((PHASES,)),
            ],
            compiler_params=pltpu.CompilerParams(collective_id=0, has_side_effects=True, vmem_limit_bytes=60 * 2**20),
        )(q, k.reshape(shape), v.reshape(shape))

    return jax.shard_map(
        step,
        mesh=mesh,
        in_specs=(P("dp", None, None), P("dp", "sp", None, None), P("dp", "sp", None, None)),
        out_specs=P("dp", None, None),
        check_vma=False,
    )
```

```python
import functools

import jax
import jax.numpy as jnp
from jax import lax
from jax.experimental import pallas as pl
from jax.experimental.pallas import tpu as pltpu
from jax.sharding import PartitionSpec as P

MESH = pl.DeviceIdType.MESH
K_SLOTS = 10
V_SLOTS = 10
GREET = 16
RUN = 2
BUFFERS = 4
FIRST = 2
PHASES = 2
LANES = 128


def distance(x):
    return bin(x >> 3).count("1") + (x >> 1 & 3)


def order_of(n):
    tail = [x for x in (2, 8, 3, 9, 16, 17, 1, 0) if x < n]
    return sorted((x for x in range(n) if x not in tail), key=lambda x: (-distance(x), -x)) + tail


def kernel(n, scale, q_hbm, k_hbm, v_hbm, out_ref, q_ref, kbuf, vbuf, s_refs, p_refs, part_out, part_in, acc_ref, top_ref, sums_ref, own_ref, qsem, ksem, vsem, part_ssem, part_rsem, out_ssem, out_rsem):
    me = lax.axis_index("sp")
    batch, tokens, phases, heads, head = k_hbm.shape
    half = tokens * heads // 2
    units = n * phases
    both_heads = phases * heads
    bits = (n - 1).bit_length()
    order = order_of(n)
    turn = [(1 - 2 * ((me // 2**b) % 2)) * 2**b for b in range(bits)]
    sizes = [1, 1] + [RUN] * ((units - 6) // RUN) + [1] * 4
    assert sum(sizes) == units
    starts = [sum(sizes[:b]) for b in range(len(sizes) + 1)]
    blocks = [list(range(a, b)) for a, b in zip(starts, starts[1:])] + [[], []]
    cuts = [0, n // 2, n - n // 4, n]

    def peer(x):
        return sum((turn[b] for b in range(bits) if x >> b & 1), me)

    def owner(u):
        return peer(order[u // phases])

    def group_of(i):
        return sum(i >= cut for cut in cuts[1:-1])

    def copy_k(u):
        slot = u % K_SLOTS
        return pltpu.make_async_copy(k_hbm.at[owner(u), :, u % phases], kbuf.at[slot], ksem.at[slot])

    def copy_v(u):
        slot = u % V_SLOTS
        return pltpu.make_async_copy(v_hbm.at[owner(u), :, u % phases], vbuf.at[slot], vsem.at[slot])

    def remote(src, dst, ssem, rsem, there):
        return pltpu.make_async_remote_copy(src, dst, ssem, rsem, device_id={"sp": there}, device_id_type=MESH)

    def send_part(i):
        remote(part_out.at[i], part_in.at[i], part_ssem, part_rsem.at[group_of(i)], peer(order[i])).start()

    q_copy = pltpu.make_async_copy(q_hbm, q_ref, qsem)
    q_copy.start()
    stream = [(copy_k, u) for u in blocks[0] + blocks[1]]
    for b in range(len(sizes)):
        stream += [(copy_k, u) for u in blocks[b + 2]] + [(copy_v, u) for u in blocks[b]]
    stream = [(copy, u) for copy, u in stream if u < (K_SLOTS if copy is copy_k else V_SLOTS)]
    for copy, u in stream[:3]:
        copy(u).start()

    barrier = pltpu.get_barrier_semaphore()
    for x in range(1, n):
        pl.semaphore_signal(barrier, inc=1, device_id={"sp": peer(x)}, device_id_type=MESH)

    for copy, u in stream[3:]:
        copy(u).start()

    rows = lax.broadcasted_iota(jnp.int32, (2 * heads, LANES), 0)
    lanes = lax.broadcasted_iota(jnp.int32, (2 * heads, LANES), 1)
    bias = jnp.where(rows % heads == lanes % heads, 0.0, -jnp.inf).astype(jnp.float32)
    sub = lax.broadcasted_iota(jnp.int32, (heads, LANES), 0)
    lane = lax.broadcasted_iota(jnp.int32, (heads, LANES), 1)
    factor = scale * 1.4426950408889634

    def scores(u):
        f = u % phases
        q = q_ref[owner(u)].astype(jnp.float32)[f * heads : (f + 1) * heads]
        zero = jnp.zeros_like(q)
        q2 = jnp.concatenate([jnp.concatenate([q, zero], 1), jnp.concatenate([zero, q], 1)], 0).astype(jnp.bfloat16)
        k = kbuf[u % K_SLOTS].reshape(2, half, head)
        k2 = jnp.concatenate([k[0], k[1]], 1)
        s_refs[u % BUFFERS][...] = lax.dot_general(q2, k2, (((1,), (1,)), ((), ())), preferred_element_type=jnp.float32)

    def weigh(u):
        i, f = divmod(u, phases)
        s_ref, p_ref = s_refs[u % BUFFERS], p_refs[u % BUFFERS]
        tiles = [s_ref[:, t : t + LANES] + bias for t in range(0, half, LANES)]
        high = functools.reduce(jnp.maximum, tiles)
        high = jnp.max(jnp.maximum(high[:heads], high[heads:]), 1, keepdims=True)
        both = jnp.concatenate([high, high], 0)
        weights = [jnp.exp2((t - both) * factor) for t in tiles]
        total = functools.reduce(jnp.add, weights)
        total = jnp.sum(total[:heads] + total[heads:], 1, keepdims=True)
        for t, w in enumerate(weights):
            p_ref[:, t * LANES : (t + 1) * LANES] = w.astype(jnp.bfloat16)
        stat = jnp.sum(jnp.where(lane == sub, high, jnp.where(lane == sub + heads, total, 0.0)), 0, keepdims=True)
        (part_in if i == n - 1 else part_out)[i, both_heads + f : both_heads + f + 1] = stat

    def values(u):
        v = vbuf[u % V_SLOTS].reshape(2, half, head)
        v2 = jnp.concatenate([v[0], v[1]], 1)
        seen = jnp.dot(p_refs[u % BUFFERS][...], v2, preferred_element_type=jnp.float32)
        return seen[:heads, :head] + seen[heads:, head:]

    def wait_group(g):
        run = pl.ds(cuts[g], min(cuts[g + 1], n - 1) - cuts[g])
        remote(part_in.at[run], part_in.at[run], part_ssem, part_rsem.at[g], me).wait_recv()

    def column(stat, first=0):
        picked = [jnp.where(lane == sub + first, stat[f : f + 1], 0.0) for f in range(phases)]
        return jnp.sum(jnp.concatenate(picked, 0), 1, keepdims=True)

    def absorb(g):
        stats = [part_in[i, both_heads:] for i in range(cuts[g], cuts[g + 1])]
        top = functools.reduce(jnp.maximum, stats)
        sums = jnp.zeros_like(top)
        acc = jnp.zeros((both_heads, head), jnp.float32)
        if g:
            old = top_ref[...]
            top = jnp.maximum(top, old)
            scaled = jnp.exp2((old - top) * factor)
            sums = pltpu.roll(scaled, heads, 1) * sums_ref[...]
            acc = acc_ref[...] * column(scaled)
        for i, stat in zip(range(cuts[g], cuts[g + 1]), stats):
            w = jnp.exp2((stat - top) * factor)
            sums += pltpu.roll(w, heads, 1) * stat
            acc += (own_ref[...] if i == n - 1 else part_in[i, :both_heads]) * column(w)
        if cuts[g + 1] == n:
            return (acc / column(sums, heads)).astype(jnp.bfloat16)
        top_ref[...], sums_ref[...], acc_ref[...] = top, sums, acc

    def refill(ks, vs):
        for u in ks:
            if u + K_SLOTS < units:
                copy_k(u + K_SLOTS).start()
        for u in vs:
            if u + V_SLOTS < units:
                copy_v(u + V_SLOTS).start()

    with jax.named_scope("wait0"):
        q_copy.wait()
        for u in blocks[0]:
            copy_k(u).wait()
    with jax.named_scope("score0"):
        for u in blocks[0]:
            scores(u)
    refill(blocks[0], [])
    with jax.named_scope("wait1"):
        for u in blocks[1]:
            copy_k(u).wait()
    with jax.named_scope("score1"):
        for u in blocks[1]:
            scores(u)
        for u in blocks[0]:
            weigh(u)

    spare = {units - 2: 0}
    sent = 0
    for b in range(len(sizes)):
        now, soon, later = blocks[b : b + 3]
        if now[0] >= GREET and not sent:
            with jax.named_scope("barrier"):
                pl.semaphore_wait(barrier, n - 1)
            for i in range(now[0] // phases):
                send_part(i)
            sent = now[0]
        refill(soon, blocks[b - 1] if b else [])
        groups = [spare[u] for u in now if u in spare]
        with jax.named_scope("wait"):
            for u in later:
                copy_k(u).wait()
            for u in now:
                copy_v(u).wait()
            for group in groups:
                wait_group(group)
        with jax.named_scope("body"):
            for u in now:
                i, f = divmod(u, phases)
                run = pl.ds(f * heads, heads)
                if i < n - 1:
                    part_out[i, run] = values(u)
                else:
                    own_ref[run] = values(u)
            for u in soon:
                weigh(u)
            for u in later:
                scores(u)
            for group in groups:
                absorb(group)
        if sent:
            for u in now:
                if u % phases == phases - 1 and u < units - phases:
                    send_part(u // phases)

    with jax.named_scope("waitparts1"):
        wait_group(1)
    with jax.named_scope("combine1"):
        absorb(1)
    with jax.named_scope("waitparts"):
        wait_group(2)
    with jax.named_scope("combine"):
        out_ref[me] = absorb(2)

    with jax.named_scope("sendout"):

        def send(there):
            remote(out_ref.at[me], out_ref.at[me], out_ssem, out_rsem, there).start()

        for there in range(FIRST):
            pl.when(me != there)(functools.partial(send, there))
        for x in order[:-1]:
            there = peer(x)
            pl.when(there >= FIRST)(functools.partial(send, there))
    with jax.named_scope("waitout"):
        landed = out_ref.at[pl.ds(0, n - 1)]
        remote(landed, landed, out_ssem, out_rsem, me).wait()
    with jax.named_scope("waitsends"):
        every = pl.ds(0, n - 1)
        remote(part_out.at[every], part_out.at[every], part_ssem, part_rsem.at[0], me).wait_send()


def solution(mesh):
    n = mesh.shape["sp"]

    def step(q, k, v):
        batch, tokens, heads, head = k.shape
        heads //= PHASES
        half = tokens * heads // 2
        shape = (batch, tokens, PHASES, heads, head)
        return pl.pallas_call(
            functools.partial(kernel, n, head**-0.5),
            out_shape=pltpu.VMEM(q.shape, q.dtype),
            in_specs=[pl.BlockSpec(memory_space=pl.ANY)] * 3,
            out_specs=pl.BlockSpec(memory_space=pltpu.VMEM),
            scratch_shapes=[
                pltpu.VMEM(q.shape, q.dtype),
                pltpu.VMEM((K_SLOTS, tokens, heads, head), k.dtype),
                pltpu.VMEM((V_SLOTS, tokens, heads, head), v.dtype),
                [pltpu.VMEM((2 * heads, half), jnp.float32)] * BUFFERS,
                [pltpu.VMEM((2 * heads, half), jnp.bfloat16)] * BUFFERS,
                pltpu.VMEM((n, PHASES * heads + PHASES, LANES), jnp.float32),
                pltpu.VMEM((n, PHASES * heads + PHASES, LANES), jnp.float32),
                pltpu.VMEM((PHASES * heads, head), jnp.float32),
                pltpu.VMEM((PHASES, LANES), jnp.float32),
                pltpu.VMEM((PHASES, LANES), jnp.float32),
                pltpu.VMEM((PHASES * heads, head), jnp.float32),
                pltpu.SemaphoreType.DMA,
                pltpu.SemaphoreType.DMA((K_SLOTS,)),
                pltpu.SemaphoreType.DMA((V_SLOTS,)),
                pltpu.SemaphoreType.DMA,
                pltpu.SemaphoreType.DMA((3,)),
                pltpu.SemaphoreType.DMA,
                pltpu.SemaphoreType.DMA,
            ],
            compiler_params=pltpu.CompilerParams(collective_id=0, has_side_effects=True, vmem_limit_bytes=60 * 2**20),
        )(q, k.reshape(shape), v.reshape(shape))

    return jax.shard_map(
        step,
        mesh=mesh,
        in_specs=(P("dp", None, None), P("dp", "sp", None, None), P("dp", "sp", None, None)),
        out_specs=P("dp", None, None),
        check_vma=False,
    )
```

```python
import functools

import jax
import jax.numpy as jnp
from jax import lax
from jax.experimental import pallas as pl
from jax.experimental.pallas import tpu as pltpu
from jax.sharding import PartitionSpec as P

MESH = pl.DeviceIdType.MESH
K_SLOTS = 10
V_SLOTS = 10
GREET = 16
RUN = 2
BUFFERS = 4
FIRST = 2
PHASES = 2
LANES = 128


def distance(x):
    return bin(x >> 3).count("1") + (x >> 1 & 3)


def order_of(n):
    tail = [x for x in (2, 8, 3, 9, 16, 17, 1, 0) if x < n]
    return sorted((x for x in range(n) if x not in tail), key=lambda x: (-distance(x), -x)) + tail


def kernel(n, scale, q_hbm, k_hbm, v_hbm, out_ref, q_ref, kbuf, vbuf, s_refs, p_refs, part_out, part_in, acc_ref, top_ref, sums_ref, own_ref, qsem, ksem, vsem, part_ssem, part_rsem, out_ssem, out_rsem):
    me = lax.axis_index("sp")
    batch, tokens, phases, heads, head = k_hbm.shape
    half = tokens * heads // 2
    units = n * phases
    both_heads = phases * heads
    bits = (n - 1).bit_length()
    order = order_of(n)
    turn = [(1 - 2 * ((me // 2**b) % 2)) * 2**b for b in range(bits)]
    sizes = [1, 1] + [RUN] * ((units - 6) // RUN) + [1] * 4
    assert sum(sizes) == units
    starts = [sum(sizes[:b]) for b in range(len(sizes) + 1)]
    blocks = [list(range(a, b)) for a, b in zip(starts, starts[1:])] + [[], []]
    cuts = [0, n // 2, n - n // 4, n - n // 8, n]

    def peer(x):
        return sum((turn[b] for b in range(bits) if x >> b & 1), me)

    def owner(u):
        return peer(order[u // phases])

    def group_of(i):
        return sum(i >= cut for cut in cuts[1:-1])

    def copy_k(u):
        slot = u % K_SLOTS
        return pltpu.make_async_copy(k_hbm.at[owner(u), :, u % phases], kbuf.at[slot], ksem.at[slot])

    def copy_v(u):
        slot = u % V_SLOTS
        return pltpu.make_async_copy(v_hbm.at[owner(u), :, u % phases], vbuf.at[slot], vsem.at[slot])

    def remote(src, dst, ssem, rsem, there):
        return pltpu.make_async_remote_copy(src, dst, ssem, rsem, device_id={"sp": there}, device_id_type=MESH)

    def send_part(i):
        remote(part_out.at[i], part_in.at[i], part_ssem, part_rsem.at[group_of(i)], peer(order[i])).start()

    q_copy = pltpu.make_async_copy(q_hbm, q_ref, qsem)
    q_copy.start()
    stream = [(copy_k, u) for u in blocks[0] + blocks[1]]
    for b in range(len(sizes)):
        stream += [(copy_k, u) for u in blocks[b + 2]] + [(copy_v, u) for u in blocks[b]]
    stream = [(copy, u) for copy, u in stream if u < (K_SLOTS if copy is copy_k else V_SLOTS)]
    for copy, u in stream[:3]:
        copy(u).start()

    barrier = pltpu.get_barrier_semaphore()
    for x in range(1, n):
        pl.semaphore_signal(barrier, inc=1, device_id={"sp": peer(x)}, device_id_type=MESH)

    for copy, u in stream[3:]:
        copy(u).start()

    rows = lax.broadcasted_iota(jnp.int32, (2 * heads, LANES), 0)
    lanes = lax.broadcasted_iota(jnp.int32, (2 * heads, LANES), 1)
    bias = jnp.where(rows % heads == lanes % heads, 0.0, -jnp.inf).astype(jnp.float32)
    sub = lax.broadcasted_iota(jnp.int32, (heads, LANES), 0)
    lane = lax.broadcasted_iota(jnp.int32, (heads, LANES), 1)
    factor = scale * 1.4426950408889634

    def scores(u):
        f = u % phases
        q = q_ref[owner(u)].astype(jnp.float32)[f * heads : (f + 1) * heads]
        zero = jnp.zeros_like(q)
        q2 = jnp.concatenate([jnp.concatenate([q, zero], 1), jnp.concatenate([zero, q], 1)], 0).astype(jnp.bfloat16)
        k = kbuf[u % K_SLOTS].reshape(2, half, head)
        k2 = jnp.concatenate([k[0], k[1]], 1)
        s_refs[u % BUFFERS][...] = lax.dot_general(q2, k2, (((1,), (1,)), ((), ())), preferred_element_type=jnp.float32)

    def weigh(u):
        i, f = divmod(u, phases)
        s_ref, p_ref = s_refs[u % BUFFERS], p_refs[u % BUFFERS]
        tiles = [s_ref[:, t : t + LANES] + bias for t in range(0, half, LANES)]
        high = functools.reduce(jnp.maximum, tiles)
        high = jnp.max(jnp.maximum(high[:heads], high[heads:]), 1, keepdims=True)
        both = jnp.concatenate([high, high], 0)
        weights = [jnp.exp2((t - both) * factor) for t in tiles]
        total = functools.reduce(jnp.add, weights)
        total = jnp.sum(total[:heads] + total[heads:], 1, keepdims=True)
        for t, w in enumerate(weights):
            p_ref[:, t * LANES : (t + 1) * LANES] = w.astype(jnp.bfloat16)
        stat = jnp.sum(jnp.where(lane == sub, high, jnp.where(lane == sub + heads, total, 0.0)), 0, keepdims=True)
        (part_in if i == n - 1 else part_out)[i, both_heads + f : both_heads + f + 1] = stat

    def values(u):
        v = vbuf[u % V_SLOTS].reshape(2, half, head)
        v2 = jnp.concatenate([v[0], v[1]], 1)
        seen = jnp.dot(p_refs[u % BUFFERS][...], v2, preferred_element_type=jnp.float32)
        return seen[:heads, :head] + seen[heads:, head:]

    def wait_group(g):
        run = pl.ds(cuts[g], min(cuts[g + 1], n - 1) - cuts[g])
        remote(part_in.at[run], part_in.at[run], part_ssem, part_rsem.at[g], me).wait_recv()

    def column(stat, first=0):
        picked = [jnp.where(lane == sub + first, stat[f : f + 1], 0.0) for f in range(phases)]
        return jnp.sum(jnp.concatenate(picked, 0), 1, keepdims=True)

    def absorb(g):
        stats = [part_in[i, both_heads:] for i in range(cuts[g], cuts[g + 1])]
        top = functools.reduce(jnp.maximum, stats)
        sums = jnp.zeros_like(top)
        acc = jnp.zeros((both_heads, head), jnp.float32)
        if g:
            old = top_ref[...]
            top = jnp.maximum(top, old)
            scaled = jnp.exp2((old - top) * factor)
            sums = pltpu.roll(scaled, heads, 1) * sums_ref[...]
            acc = acc_ref[...] * column(scaled)
        for i, stat in zip(range(cuts[g], cuts[g + 1]), stats):
            w = jnp.exp2((stat - top) * factor)
            sums += pltpu.roll(w, heads, 1) * stat
            acc += (own_ref[...] if i == n - 1 else part_in[i, :both_heads]) * column(w)
        if cuts[g + 1] == n:
            return (acc / column(sums, heads)).astype(jnp.bfloat16)
        top_ref[...], sums_ref[...], acc_ref[...] = top, sums, acc

    def refill(ks, vs):
        for u in ks:
            if u + K_SLOTS < units:
                copy_k(u + K_SLOTS).start()
        for u in vs:
            if u + V_SLOTS < units:
                copy_v(u + V_SLOTS).start()

    with jax.named_scope("wait0"):
        q_copy.wait()
        for u in blocks[0]:
            copy_k(u).wait()
    with jax.named_scope("score0"):
        for u in blocks[0]:
            scores(u)
    refill(blocks[0], [])
    with jax.named_scope("wait1"):
        for u in blocks[1]:
            copy_k(u).wait()
    with jax.named_scope("score1"):
        for u in blocks[1]:
            scores(u)
        for u in blocks[0]:
            weigh(u)

    spare = {units - 2: 0, units - 1: 1}
    sent = 0
    for b in range(len(sizes)):
        now, soon, later = blocks[b : b + 3]
        if now[0] >= GREET and not sent:
            with jax.named_scope("barrier"):
                pl.semaphore_wait(barrier, n - 1)
            for i in range(now[0] // phases):
                send_part(i)
            sent = now[0]
        refill(soon, blocks[b - 1] if b else [])
        groups = [spare[u] for u in now if u in spare]
        with jax.named_scope("wait"):
            for u in later:
                copy_k(u).wait()
            for u in now:
                copy_v(u).wait()
            for group in groups:
                wait_group(group)
        with jax.named_scope("body"):
            for u in now:
                i, f = divmod(u, phases)
                run = pl.ds(f * heads, heads)
                if i < n - 1:
                    part_out[i, run] = values(u)
                else:
                    own_ref[run] = values(u)
            for u in soon:
                weigh(u)
            for u in later:
                scores(u)
            for group in groups:
                absorb(group)
        if sent:
            for u in now:
                if u % phases == phases - 1 and u < units - phases:
                    send_part(u // phases)

    with jax.named_scope("waitparts1"):
        wait_group(2)
    with jax.named_scope("combine1"):
        absorb(2)
    with jax.named_scope("waitparts"):
        wait_group(3)
    with jax.named_scope("combine"):
        out_ref[me] = absorb(3)

    with jax.named_scope("sendout"):

        def send(there):
            remote(out_ref.at[me], out_ref.at[me], out_ssem, out_rsem, there).start()

        for there in range(FIRST):
            pl.when(me != there)(functools.partial(send, there))
        for x in order[:-1]:
            there = peer(x)
            pl.when(there >= FIRST)(functools.partial(send, there))
    with jax.named_scope("waitout"):
        landed = out_ref.at[pl.ds(0, n - 1)]
        remote(landed, landed, out_ssem, out_rsem, me).wait()
    with jax.named_scope("waitsends"):
        every = pl.ds(0, n - 1)
        remote(part_out.at[every], part_out.at[every], part_ssem, part_rsem.at[0], me).wait_send()


def solution(mesh):
    n = mesh.shape["sp"]

    def step(q, k, v):
        batch, tokens, heads, head = k.shape
        heads //= PHASES
        half = tokens * heads // 2
        shape = (batch, tokens, PHASES, heads, head)
        return pl.pallas_call(
            functools.partial(kernel, n, head**-0.5),
            out_shape=pltpu.VMEM(q.shape, q.dtype),
            in_specs=[pl.BlockSpec(memory_space=pl.ANY)] * 3,
            out_specs=pl.BlockSpec(memory_space=pltpu.VMEM),
            scratch_shapes=[
                pltpu.VMEM(q.shape, q.dtype),
                pltpu.VMEM((K_SLOTS, tokens, heads, head), k.dtype),
                pltpu.VMEM((V_SLOTS, tokens, heads, head), v.dtype),
                [pltpu.VMEM((2 * heads, half), jnp.float32)] * BUFFERS,
                [pltpu.VMEM((2 * heads, half), jnp.bfloat16)] * BUFFERS,
                pltpu.VMEM((n, PHASES * heads + PHASES, LANES), jnp.float32),
                pltpu.VMEM((n, PHASES * heads + PHASES, LANES), jnp.float32),
                pltpu.VMEM((PHASES * heads, head), jnp.float32),
                pltpu.VMEM((PHASES, LANES), jnp.float32),
                pltpu.VMEM((PHASES, LANES), jnp.float32),
                pltpu.VMEM((PHASES * heads, head), jnp.float32),
                pltpu.SemaphoreType.DMA,
                pltpu.SemaphoreType.DMA((K_SLOTS,)),
                pltpu.SemaphoreType.DMA((V_SLOTS,)),
                pltpu.SemaphoreType.DMA,
                pltpu.SemaphoreType.DMA((4,)),
                pltpu.SemaphoreType.DMA,
                pltpu.SemaphoreType.DMA,
            ],
            compiler_params=pltpu.CompilerParams(collective_id=0, has_side_effects=True, vmem_limit_bytes=60 * 2**20),
        )(q, k.reshape(shape), v.reshape(shape))

    return jax.shard_map(
        step,
        mesh=mesh,
        in_specs=(P("dp", None, None), P("dp", "sp", None, None), P("dp", "sp", None, None)),
        out_specs=P("dp", None, None),
        check_vma=False,
    )
```
